32 devices in a mesh: gx: 4 (over y, core), gy: 8 (over z, x).
Axes of the slice: x: 2, y: 2, z: 4, core: 2. Of those that a mesh axis runs over, the one named last changes fastest.
Arguments:
- hidden_states: bfloat16 [1024, 128], replicated, may hold values from -60 to 60
- item_table: bfloat16 [262144, 128], P(('gx', 'gy')), may hold values from -1.796875 to 1.796875
- targets: int32 [1024], replicated, may hold values from 0 to 262143
Outputs:
- expected: float32 [1024, 128], P(('gx', 'gy'))
- nll: float32 [1024], P(('gx', 'gy'))
The draws below stay inside these ranges and needn't reach their ends.
All inputs are finite; a program needn't handle non-finite values.
Results may differ from the reference program's by a relative error of at most 0.0023.
Values sent between devices are 32-bit elements; how exact they have to be, the bound alone decides.
No kernel may reach another device: no remote copies, remote signals or barrier semaphores. Data moves between devices by JAX's collectives and lax.ppermute only.
A program may use at most 64 MiB of HBM per device.

```python
import jax
import jax.numpy as jnp
from jax import lax

D = 128
BLK = 512
P_SIZE = 1024
ITEMS = 262144


def draw_hidden_states(key, part):
    first_key = jax.random.fold_in(jax.random.fold_in(key, 17), 0)
    normal_draw = jax.random.normal(first_key, (P_SIZE, D), jnp.float32)
    result_rows = jnp.clip(normal_draw, -6.0, 6.0)
    return result_rows.astype(jnp.bfloat16)


def plant(entries, own_key, smallest, high):
    longest = entries.shape.index(max(entries.shape))
    spots = []
    for shift in (0, 1):
        where = [jax.random.randint(jax.random.fold_in(own_key, axis), (), 0, length) for axis, length in enumerate(entries.shape)]
        where[longest] = (where[longest] + shift) % entries.shape[longest]
        spots.append(tuple(where))
    return entries.at[spots[0]].set(smallest).at[spots[1]].set(high)


def shard_levels(stream_key, dims, shards, low, largest):
    def one(dim, shards_of):
        draws = jax.random.uniform(jax.random.fold_in(jax.random.fold_in(stream_key, 6), dim), (shards_of,), jnp.float32, low / len(shards), largest / len(shards))
        return jnp.repeat(jnp.exp(draws), dims[dim] // shards_of).reshape((-1,) + (1,) * (len(dims) - dim - 1))

    factor_of = one(*shards[0])
    for cut in shards[1:]:
        factor_of = factor_of * one(*cut)
    return factor_of


def normal_values(rng, dims, spread, limit, pieces=(), dtype=jnp.bfloat16):
    gain = shard_levels(rng, dims, pieces, -0.22, 0.18) if pieces else 1.0
    entries = jax.random.normal(rng, dims, jnp.float32) * spread * gain
    return jnp.minimum(jnp.maximum(entries, -limit), limit).astype(dtype)


def setup_inputs(seed: int = 0) -> dict:
    key_list = jax.random.split(jax.random.key(seed), 4)
    return {
        "hidden_states": draw_hidden_states(jax.random.fold_in(key_list[3], 71), 0),
        "item_table": normal_values(key_list[1], (ITEMS, D), 0.3, 1.796875, ((0, 32),)),
        "targets": plant(jax.random.randint(key_list[2], (P_SIZE,), 0, ITEMS), jax.random.fold_in(key_list[2], 1), 0, ITEMS - 1).astype(jnp.int32),
    }


def reference(hidden_states, item_table, targets):
    nblocks = item_table.shape[0] // BLK
    blocks = item_table.reshape(nblocks, BLK, D)

    def visit_block(carry, block):
        highest, totals, weighted = carry
        scores = lax.dot_general(hidden_states, block, (((1,), (1,)), ((), ())), preferred_element_type=jnp.float32)
        block_max = jnp.max(scores, axis=1)
        exponent = jnp.exp(scores - block_max[:, None])
        block_sum = jnp.sum(exponent, axis=1)
        probs_low = exponent.astype(jnp.bfloat16)
        block_acc = jnp.dot(probs_low, block, preferred_element_type=jnp.float32)
        new_max = jnp.maximum(highest, block_max)
        retain = jnp.exp(highest - new_max)
        rescale = jnp.exp(block_max - new_max)
        totals = totals * retain + block_sum * rescale
        weighted = weighted * retain[:, None] + block_acc * rescale[:, None]
        return (new_max, totals, weighted), None

    start_state = (jnp.full((P_SIZE,), -1e30, jnp.float32), jnp.zeros((P_SIZE,), jnp.float32), jnp.zeros((P_SIZE, D), jnp.float32))
    (highest, totals, weighted), unused_out = lax.scan(visit_block, start_state, blocks)
    target_rows = item_table[targets]
    target_logit = jnp.sum(hidden_states.astype(jnp.float32) * target_rows.astype(jnp.float32), axis=1)
    expected = weighted / totals[:, None]
    nll = highest + jnp.log(totals) - target_logit
    return expected, nll
```

```python
import jax
import jax.numpy as jnp
from jax import lax
from jax.sharding import PartitionSpec as P

BLK = 512


def local(hidden_states, item_table, targets):
    positions = hidden_states.shape[0]
    shard_items = item_table.shape[0]
    nblocks = shard_items // BLK

    def visit_block(block_index, carry):
        highest, totals, weighted = carry
        block = lax.dynamic_slice_in_dim(item_table, block_index * BLK, BLK, 0)
        scores = lax.dot_general(
            hidden_states, block, (((1,), (1,)), ((), ())), preferred_element_type=jnp.float32
        )
        block_max = jnp.max(scores, axis=1)
        exponent = jnp.exp(scores - block_max[:, None])
        block_sum = jnp.sum(exponent, axis=1)
        probs_low = exponent.astype(jnp.bfloat16)
        block_acc = jnp.dot(probs_low, block, preferred_element_type=jnp.float32)
        new_max = jnp.maximum(highest, block_max)
        retain = jnp.exp(highest - new_max)
        rescale = jnp.exp(block_max - new_max)
        totals = totals * retain + block_sum * rescale
        weighted = weighted * retain[:, None] + block_acc * rescale[:, None]
        return (new_max, totals, weighted)

    start_state = (
        jnp.full((positions,), -1e30, jnp.float32),
        jnp.zeros((positions,), jnp.float32),
        jnp.zeros((positions, item_table.shape[1]), jnp.float32),
    )
    highest, totals, weighted = lax.fori_loop(0, nblocks, visit_block, start_state)
    device_index = lax.axis_index(("gx", "gy"))
    local_index = targets - device_index * shard_items
    owner_mask = (local_index >= 0) & (local_index < shard_items)
    target_rows = item_table[jnp.clip(local_index, 0, shard_items - 1)]
    own_logit = jnp.sum(hidden_states.astype(jnp.float32) * target_rows.astype(jnp.float32), axis=1)
    own_logit = jnp.where(owner_mask, own_logit, 0.0)
    devices = lax.axis_size(("gx", "gy"))
    rows = positions // devices
    stats = jnp.stack([highest, totals, own_logit]).reshape(3, devices, rows)
    stats = jnp.transpose(stats, (1, 0, 2)).reshape(devices, 3 * rows)
    lanes = item_table.shape[1]
    extra = -(-3 * rows // lanes)
    stats = jnp.pad(stats, ((0, 0), (0, extra * lanes - 3 * rows)))
    payload = jnp.concatenate(
        [weighted.reshape(devices, rows, lanes), stats.reshape(devices, extra, lanes)], axis=1
    )
    got = lax.all_to_all(payload, ("gx", "gy"), 0, 0, tiled=True)
    parts = got[:, rows:].reshape(devices, extra * lanes)
    part_max = parts[:, :rows]
    max_rows = jnp.max(part_max, axis=0)
    factor = jnp.exp(part_max - max_rows[None])
    total_rows = jnp.sum(parts[:, rows:2 * rows] * factor, axis=0)
    target_rows = jnp.sum(parts[:, 2 * rows:3 * rows], axis=0)
    weighted_rows = jnp.sum(got[:, :rows] * factor[:, :, None], axis=0)
    expected = weighted_rows / total_rows[:, None]
    nll = max_rows + jnp.log(total_rows) - target_rows
    return (expected, nll)


def solution(mesh):
    return jax.shard_map(
        local,
        mesh=mesh,
        in_specs=(P(), P(("gx", "gy"), None), P()),
        out_specs=(P(("gx", "gy"), None), P(("gx", "gy"))),
        check_vma=False,
    )
```

```python
import jax
import jax.numpy as jnp
from jax import lax
from jax.experimental import pallas as pl
from jax.experimental.pallas import tpu as pltpu
from jax.sharding import PartitionSpec as P

AXES = ("gx", "gy")
POS_TILE = 512
ITEM_TILE = 1024


def tile_of(size, tile):
    while size % tile:
        tile //= 2
    return tile


def softmax_kernel(hidden_ref, table_ref, local_ref, acc_ref, stats_ref, *, item_tile):
    hidden = hidden_ref[...]
    positions, lanes = acc_ref.shape
    wanted = jnp.broadcast_to(local_ref[...], (128, positions)).T
    lane = lax.broadcasted_iota(jnp.int32, (positions, 128), 1)
    wanted = wanted - lane
    picked = jnp.zeros((positions, 128), jnp.float32)
    highest = None
    for first in range(0, table_ref.shape[0], item_tile):
        block = table_ref[first:first + item_tile, :]
        scores = lax.dot_general(
            hidden, block, (((1,), (1,)), ((), ())), preferred_element_type=jnp.float32
        )
        for col in range(0, item_tile, 128):
            picked = jnp.where(wanted == first + col, scores[:, col:col + 128], picked)
        new_max = jnp.max(scores, axis=1, keepdims=True)
        if highest is not None:
            new_max = jnp.maximum(highest, new_max)
        probs = jnp.exp(scores - new_max)
        sums = jnp.sum(probs, axis=1, keepdims=True)
        products = jnp.dot(probs.astype(jnp.bfloat16), block, preferred_element_type=jnp.float32)
        if highest is None:
            totals, weighted = sums, products
        else:
            retain = jnp.exp(highest - new_max)
            totals = totals * retain + sums
            weighted = weighted * retain + products
        highest = new_max
    acc_ref[...] = weighted
    logit = jnp.sum(picked, axis=1, keepdims=True)
    stats = jnp.where(lane == 0, highest, jnp.where(lane == 1, totals, logit))
    stats_ref[...] = stats.T[:8]


def local_softmax(hidden_states, item_table, local_index):
    positions, width = hidden_states.shape
    pos_tile = tile_of(positions, POS_TILE)
    item_tile = tile_of(item_table.shape[0], ITEM_TILE)

    def body(*refs):
        softmax_kernel(*refs, item_tile=item_tile)

    return pl.pallas_call(
        body,
        name="block_softmax",
        grid=(positions // pos_tile,),
        in_specs=[
            pl.BlockSpec((pos_tile, width), lambda i: (i, 0)),
            pl.BlockSpec(item_table.shape, lambda i: (0, 0)),
            pl.BlockSpec((1, pos_tile), lambda i: (0, i)),
        ],
        out_specs=[
            pl.BlockSpec((pos_tile, width), lambda i: (i, 0)),
            pl.BlockSpec((8, pos_tile), lambda i: (0, i)),
        ],
        out_shape=[
            jax.ShapeDtypeStruct((positions, width), jnp.float32),
            jax.ShapeDtypeStruct((8, positions), jnp.float32),
        ],
    )(hidden_states, item_table, local_index[None])


def local(hidden_states, item_table, targets):
    positions, lanes = hidden_states.shape
    device_index = lax.axis_index(AXES)
    local_index = targets - device_index * item_table.shape[0]
    weighted, stats = local_softmax(hidden_states, item_table, local_index)
    devices = lax.axis_size(AXES)
    rows = positions // devices
    stats = stats[:3].reshape(3, devices, rows)
    stats = jnp.transpose(stats, (1, 0, 2)).reshape(devices, 3 * rows)
    extra = -(-3 * rows // lanes)
    stats = jnp.pad(stats, ((0, 0), (0, extra * lanes - 3 * rows)))
    payload = jnp.concatenate(
        [weighted.reshape(devices, rows, lanes), stats.reshape(devices, extra, lanes)], axis=1
    )
    got = lax.all_to_all(payload, AXES, 0, 0, tiled=True)
    parts = got[:, rows:].reshape(devices, extra * lanes)
    part_max = parts[:, :rows]
    max_rows = jnp.max(part_max, axis=0)
    factor = jnp.exp(part_max - max_rows[None])
    total_rows = jnp.sum(parts[:, rows:2 * rows] * factor, axis=0)
    target_rows = jnp.sum(parts[:, 2 * rows:3 * rows], axis=0)
    weighted_rows = jnp.sum(got[:, :rows] * factor[:, :, None], axis=0)
    expected = weighted_rows / total_rows[:, None]
    nll = max_rows + jnp.log(total_rows) - target_rows
    return (expected, nll)


def solution(mesh):
    return jax.shard_map(
        local,
        mesh=mesh,
        in_specs=(P(), P(AXES, None), P()),
        out_specs=(P(AXES, None), P(AXES)),
        check_vma=False,
    )
```

```python
import jax
import jax.numpy as jnp
from jax import lax
from jax.experimental import pallas as pl
from jax.experimental.pallas import tpu as pltpu
from jax.sharding import PartitionSpec as P

AXES = ("gx", "gy")
ITEM_TILE = 1024


def tile_of(size, tile):
    while size % tile:
        tile //= 2
    return tile


def softmax_kernel(place_ref, hidden_ref, table_ref, targets_ref, out_ref, *, item_tile):
    groups, _, run, width = hidden_ref.shape
    positions = groups * run
    rows = positions // out_ref.shape[0]
    hidden = hidden_ref[...].reshape(positions, width)
    half = place_ref[0]
    wanted = jnp.concatenate(
        [
            jnp.broadcast_to(
                targets_ref[:, pl.ds(pl.multiple_of((2 * g + half) * run, 128), run)], (128, run)
            ).T
            for g in range(groups)
        ],
        axis=0,
    ) - place_ref[1]
    lane = lax.broadcasted_iota(jnp.int32, (positions, 128), 1)
    wanted = wanted - lane
    picked = jnp.zeros((positions, 128), jnp.float32)
    highest = None
    for first in range(0, table_ref.shape[0], item_tile):
        block = table_ref[first:first + item_tile, :]
        scores = lax.dot_general(
            hidden, block, (((1,), (1,)), ((), ())), preferred_element_type=jnp.float32
        )
        for col in range(0, item_tile, 128):
            picked = jnp.where(wanted == first + col, scores[:, col:col + 128], picked)
        new_max = jnp.max(scores, axis=1, keepdims=True)
        if highest is not None:
            new_max = jnp.maximum(highest, new_max)
        probs = jnp.exp(scores - new_max)
        sums = jnp.sum(probs, axis=1, keepdims=True)
        products = jnp.dot(probs.astype(jnp.bfloat16), block, preferred_element_type=jnp.float32)
        if highest is None:
            totals, weighted = sums, products
        else:
            retain = jnp.exp(highest - new_max)
            totals = totals * retain + sums
            weighted = weighted * retain + products
        highest = new_max
    logit = jnp.sum(picked, axis=1, keepdims=True)
    slot = lane - lax.broadcasted_iota(jnp.int32, (positions, 128), 0) % rows
    stats = jnp.where(slot == 0, highest, 0.0)
    stats = jnp.where(slot == rows, totals, stats)
    stats = jnp.where(slot == 2 * rows, logit, stats)
    out_ref[:, :rows, :] = weighted.reshape(-1, rows, width)
    out_ref[:, rows:, :] = jnp.sum(stats.reshape(-1, rows, 128), axis=1, keepdims=True)


def half_softmax(hidden_states, item_table, targets, half, first_item, pairs, devices):
    positions, width = hidden_states.shape
    rows = positions // devices
    run = positions // (2 * pairs)
    item_tile = tile_of(item_table.shape[0], ITEM_TILE)

    def body(*refs):
        softmax_kernel(*refs, item_tile=item_tile)

    return pl.pallas_call(
        body,
        name="half_softmax",
        grid_spec=pltpu.PrefetchScalarGridSpec(
            num_scalar_prefetch=1,
            grid=(1,),
            in_specs=[
                pl.BlockSpec((pairs, 1, run, width), lambda i, place: (0, place[0], 0, 0)),
                pl.BlockSpec(item_table.shape, lambda i, place: (0, 0)),
                pl.BlockSpec((1, positions), lambda i, place: (0, 0)),
            ],
            out_specs=pl.BlockSpec((devices // 2, rows + 1, width), lambda i, place: (0, 0, 0)),
        ),
        out_shape=jax.ShapeDtypeStruct((devices // 2, rows + 1, width), jnp.float32),
    )(
        jnp.stack([half, first_item]),
        hidden_states.reshape(pairs, 2, run, width),
        item_table,
        targets[None],
    )


def local(hidden_states, item_table, targets):
    outer, inner = lax.axis_size("gx"), lax.axis_size("gy")
    devices, pairs = outer * inner, outer // 2
    rows = hidden_states.shape[0] // devices
    device_index = lax.axis_index(AXES)
    first_item = device_index * item_table.shape[0]
    own = lax.axis_index("gx") % 2

    def run(half):
        return half_softmax(hidden_states, item_table, targets, half, first_item, pairs, devices)

    sent = run(1 - own)
    other = lax.ppermute(sent, "gx", [(i, i ^ 1) for i in range(outer)])
    kept = run(own)
    kept_max, other_max = kept[:, rows, :rows], other[:, rows, :rows]
    pair_max = jnp.maximum(kept_max, other_max)
    kept_factor, other_factor = jnp.exp(kept_max - pair_max), jnp.exp(other_max - pair_max)
    weighted = kept[:, :rows] * kept_factor[:, :, None] + other[:, :rows] * other_factor[:, :, None]
    totals = (
        kept[:, rows, rows:2 * rows] * kept_factor + other[:, rows, rows:2 * rows] * other_factor
    )
    logits = kept[:, rows, 2 * rows:3 * rows] + other[:, rows, 2 * rows:3 * rows]
    stats = jnp.concatenate([pair_max, totals, logits], axis=1)
    stats = jnp.pad(stats, ((0, 0), (0, weighted.shape[2] - 3 * rows)))
    payload = jnp.concatenate([weighted, stats[:, None]], axis=1)
    members = [
        [(2 * p + c) * inner + g for p in range(pairs) for g in range(inner)] for c in range(2)
    ]
    got = lax.all_to_all(payload, AXES, 0, 0, axis_index_groups=members, tiled=True)
    parts = got[:, rows]
    part_max = parts[:, :rows]
    max_rows = jnp.max(part_max, axis=0)
    factor = jnp.exp(part_max - max_rows[None])
    total_rows = jnp.sum(parts[:, rows:2 * rows] * factor, axis=0)
    target_rows = jnp.sum(parts[:, 2 * rows:3 * rows], axis=0)
    weighted_rows = jnp.sum(got[:, :rows] * factor[:, :, None], axis=0)
    expected = weighted_rows / total_rows[:, None]
    nll = max_rows + jnp.log(total_rows) - target_rows
    return (expected, nll)


def solution(mesh):
    return jax.shard_map(
        local,
        mesh=mesh,
        in_specs=(P(), P(AXES, None), P()),
        out_specs=(P(AXES, None), P(AXES)),
        check_vma=False,
    )
```

```python
import jax
import jax.numpy as jnp
from jax import lax
from jax.experimental import pallas as pl
from jax.experimental.pallas import tpu as pltpu
from jax.sharding import PartitionSpec as P

AXES = ("gx", "gy")
ITEM_TILE = 2048


def tile_of(size, tile):
    while size % tile:
        tile //= 2
    return tile


def softmax_kernel(place_ref, hidden_ref, table_ref, targets_ref, out_ref, *, item_tile, turn):
    groups, _, run, width = hidden_ref.shape
    positions = groups * run
    rows = positions // out_ref.shape[0]
    hidden = hidden_ref[...].reshape(positions, width)
    half = place_ref[turn]
    wanted = jnp.concatenate(
        [
            jnp.broadcast_to(
                targets_ref[:, pl.ds(pl.multiple_of((2 * g + half) * run, 128), run)], (128, run)
            ).T
            for g in range(groups)
        ],
        axis=0,
    ) - place_ref[2]
    lane = lax.broadcasted_iota(jnp.int32, (positions, 128), 1)
    wanted = wanted - lane
    picked = jnp.zeros((positions, 128), jnp.float32)
    highest = None
    for first in range(0, table_ref.shape[0], item_tile):
        block = table_ref[first:first + item_tile, :]
        scores = lax.dot_general(
            hidden, block, (((1,), (1,)), ((), ())), preferred_element_type=jnp.float32
        )
        for col in range(0, item_tile, 128):
            picked = jnp.where(wanted == first + col, scores[:, col:col + 128], picked)
        new_max = jnp.max(scores, axis=1, keepdims=True)
        if highest is not None:
            new_max = jnp.maximum(highest, new_max)
        probs = jnp.exp(scores - new_max)
        sums = jnp.sum(probs, axis=1, keepdims=True)
        products = jnp.dot(probs.astype(jnp.bfloat16), block, preferred_element_type=jnp.float32)
        if highest is None:
            totals, weighted = sums, products
        else:
            retain = jnp.exp(highest - new_max)
            totals = totals * retain + sums
            weighted = weighted * retain + products
        highest = new_max
    logit = jnp.sum(picked, axis=1, keepdims=True)
    slot = lane - lax.broadcasted_iota(jnp.int32, (positions, 128), 0) % rows
    stats = jnp.where(slot == 0, highest, 0.0)
    stats = jnp.where(slot == rows, totals, stats)
    stats = jnp.where(slot == 2 * rows, logit, stats)
    out_ref[:, :rows, :] = weighted.reshape(-1, rows, width)
    out_ref[:, rows:, :] = jnp.sum(stats.reshape(-1, rows, 128), axis=1, keepdims=True)


def half_softmax(hidden_states, item_table, targets, place, turn, pairs, devices):
    positions, width = hidden_states.shape
    rows = positions // devices
    run = positions // (2 * pairs)
    item_tile = tile_of(item_table.shape[0], ITEM_TILE)

    def body(*refs):
        softmax_kernel(*refs, item_tile=item_tile, turn=turn)

    return pl.pallas_call(
        body,
        name="half_softmax",
        grid_spec=pltpu.PrefetchScalarGridSpec(
            num_scalar_prefetch=1,
            grid=(1,),
            in_specs=[
                pl.BlockSpec((pairs, 1, run, width), lambda i, place: (0, place[turn], 0, 0)),
                pl.BlockSpec(item_table.shape, lambda i, place: (0, 0)),
                pl.BlockSpec((1, positions), lambda i, place: (0, 0)),
            ],
            out_specs=pl.BlockSpec((devices // 2, rows + 1, width), lambda i, place: (0, 0, 0)),
        ),
        out_shape=jax.ShapeDtypeStruct((devices // 2, rows + 1, width), jnp.float32),
    )(
        place,
        hidden_states.reshape(pairs, 2, run, width),
        item_table,
        targets[None],
    )


def local(hidden_states, item_table, targets):
    outer, inner = lax.axis_size("gx"), lax.axis_size("gy")
    devices, pairs = outer * inner, outer // 2
    rows = hidden_states.shape[0] // devices
    device_index = lax.axis_index(AXES)
    first_item = device_index * item_table.shape[0]
    own = lax.axis_index("gx") % 2

    place = jnp.stack([1 - own, own, first_item])

    def run(turn):
        return half_softmax(hidden_states, item_table, targets, place, turn, pairs, devices)

    sent = run(0)
    other = lax.ppermute(sent, "gx", [(i, i ^ 1) for i in range(outer)])
    kept = run(1)
    kept_max, other_max = kept[:, rows, :rows], other[:, rows, :rows]
    pair_max = jnp.maximum(kept_max, other_max)
    kept_factor, other_factor = jnp.exp(kept_max - pair_max), jnp.exp(other_max - pair_max)
    weighted = kept[:, :rows] * kept_factor[:, :, None] + other[:, :rows] * other_factor[:, :, None]
    totals = (
        kept[:, rows, rows:2 * rows] * kept_factor + other[:, rows, rows:2 * rows] * other_factor
    )
    logits = kept[:, rows, 2 * rows:3 * rows] + other[:, rows, 2 * rows:3 * rows]
    stats = jnp.concatenate([pair_max, totals, logits], axis=1)
    stats = jnp.pad(stats, ((0, 0), (0, weighted.shape[2] - 3 * rows)))
    payload = jnp.concatenate([weighted, stats[:, None]], axis=1)
    members = [
        [(2 * p + c) * inner + g for p in range(pairs) for g in range(inner)] for c in range(2)
    ]
    got = lax.all_to_all(payload, AXES, 0, 0, axis_index_groups=members, tiled=True)
    parts = got[:, rows]
    part_max = parts[:, :rows]
    max_rows = jnp.max(part_max, axis=0)
    factor = jnp.exp(part_max - max_rows[None])
    total_rows = jnp.sum(parts[:, rows:2 * rows] * factor, axis=0)
    target_rows = jnp.sum(parts[:, 2 * rows:3 * rows], axis=0)
    weighted_rows = jnp.sum(got[:, :rows] * factor[:, :, None], axis=0)
    expected = weighted_rows / total_rows[:, None]
    nll = max_rows + jnp.log(total_rows) - target_rows
    return (expected, nll)


def solution(mesh):
    return jax.shard_map(
        local,
        mesh=mesh,
        in_specs=(P(), P(AXES, None), P()),
        out_specs=(P(AXES, None), P(AXES)),
        check_vma=False,
    )
```
